32 devices in a mesh: bank: 4 (over y, x), zero: 8 (over z, core).
Axes of the slice: x: 2, y: 2, z: 4, core: 2. Of those that a mesh axis runs over, the one named last changes fastest.
Arguments:
- master_gate: float32 [64, 2048, 1408], P('bank', 'zero'), may hold values from -0.1875 to 0.1875
- master_up: float32 [64, 2048, 1408], P('bank', 'zero'), may hold values from -0.1875 to 0.1875
- master_down: float32 [64, 1408, 2048], P('bank', None, 'zero'), may hold values from -0.21875 to 0.21875
- router_weight: float32 [2048, 64], P('zero', 'bank'), may hold values from -0.125 to 0.125
- router_gain: float32 [2048], P('zero'), may hold values from 0.25 to 1.75
Outputs:
- final_gate: bfloat16 [64, 2048, 1408], P('bank', None, 'zero')
- final_up: bfloat16 [64, 2048, 1408], P('bank', None, 'zero')
- final_down: bfloat16 [64, 1408, 2048], P('bank', 'zero')
- scale_gate: float32 [64, 1408], P('bank', 'zero')
- scale_up: float32 [64, 1408], P('bank', 'zero')
- scale_down: float32 [64, 1408], P('bank', 'zero')
- serve_router: bfloat16 [2048, 64], replicated
The draws below stay inside these ranges and needn't reach their ends.
All inputs are finite; a program needn't handle non-finite values. Where the reference program divides by a largest or mean magnitude, that divisor is 1e-20 or more.
Results may differ from the reference program's by a relative error of at most 0.001.
Values may be sent and summed in bfloat16 or wider, within the bound.
A program may use at most 256 MiB of HBM per device.

```python
import jax
import jax.numpy as jnp

EXPERTS = 64
D_MODEL = 2048
D_EXPERT = 1408


def strengthened(array, rng, source, target, parts, factor):
    def block_of(dim):
        return (jnp.arange(array.shape[dim]) // (array.shape[dim] // parts)).reshape((-1,) + (1,) * (array.ndim - 1 - dim))

    one_side = jax.random.permutation(rng, parts)[block_of(target)]
    second = (block_of(target) + parts // 2) % parts
    return jnp.where((block_of(source) == one_side) | (block_of(source) == second), factor * array, array)


def level_of(stream_key, extent, pieces, least, top_value):
    def one(axis_at, parts):
        heights = jax.random.uniform(jax.random.fold_in(jax.random.fold_in(stream_key, 6), axis_at), (parts,), jnp.float32, least / len(pieces), top_value / len(pieces))
        return jnp.repeat(jnp.exp(heights), extent[axis_at] // parts).reshape((-1,) + (1,) * (len(extent) - axis_at - 1))

    level = one(*pieces[0])
    for cut in pieces[1:]:
        level = level * one(*cut)
    return level


def bell_draw(rng, shape, spread, most, pieces=(), dtype=jnp.bfloat16):
    loudness = level_of(rng, shape, pieces, -0.22, 0.18) if pieces else 1.0
    result = jax.random.normal(rng, shape, jnp.float32) * spread * loudness
    return jnp.minimum(jnp.maximum(result, -most), most).astype(dtype)


def noise_with(own_key, extent, spread, most, cuts, heavy, dtype=jnp.bfloat16):
    result = spread * jax.random.normal(own_key, extent, jnp.float32)
    if cuts:
        result = result * level_of(own_key, extent, cuts, -0.22, 0.18)
    return jnp.clip(strengthened(result, jax.random.fold_in(own_key, 3), *heavy), -most, most).astype(dtype)


def setup_inputs(seed: int = 0) -> dict:
    keys = jax.random.split(jax.random.key(seed), 6)
    return {
        "master_gate": noise_with(keys[0], (EXPERTS, D_MODEL, D_EXPERT), D_MODEL ** -0.5, 0.1875, ((0, 4), (1, 8)), (1, 2, 8, 2.0), jnp.float32),
        "master_up": noise_with(keys[1], (EXPERTS, D_MODEL, D_EXPERT), D_MODEL ** -0.5, 0.1875, ((0, 4), (1, 8)), (1, 2, 8, 2.0), jnp.float32),
        "master_down": noise_with(keys[2], (EXPERTS, D_EXPERT, D_MODEL), D_EXPERT ** -0.5, 0.21875, ((0, 4), (2, 8)), (2, 1, 8, 2.0), jnp.float32),
        "router_weight": bell_draw(keys[3], (D_MODEL, EXPERTS), D_MODEL ** -0.5, 0.125, ((0, 8), (1, 4)), jnp.float32),
        "router_gain": jnp.clip(1.0 + 0.15 * jax.random.normal(keys[4], (D_MODEL,), jnp.float32), 0.25, 1.75),
    }


def reference(master_gate, master_up, master_down, router_weight, router_gain):
    scale_gate = jnp.max(jnp.abs(master_gate), axis=1)
    final_gate = (master_gate / jnp.expand_dims(scale_gate, 1)).astype(jnp.bfloat16)
    scale_up = jnp.max(jnp.abs(master_up), axis=1)
    final_up = (master_up / jnp.expand_dims(scale_up, 1)).astype(jnp.bfloat16)
    scale_down = jnp.max(jnp.abs(master_down), axis=2)
    final_down = (master_down / jnp.expand_dims(scale_down, 2)).astype(jnp.bfloat16)
    serve_router = (router_weight * router_gain[:, None]).astype(jnp.bfloat16)
    return final_gate, final_up, final_down, scale_gate, scale_up, scale_down, serve_router
```

```python
import functools

import jax
import jax.numpy as jnp
from jax import lax
from jax.experimental import pallas as pl
from jax.experimental.pallas import tpu as pltpu
from jax.sharding import PartitionSpec as P

MESH = pl.DeviceIdType.MESH
LANES = 128
LATE = 2
SLOTS = 3


def plain_shards(master_gate, master_up, master_down, router_weight, router_gain):
    scale_gate, scale_up, scale_down = lax.pmax(
        (
            jnp.max(jnp.abs(master_gate), axis=1),
            jnp.max(jnp.abs(master_up), axis=1),
            jnp.max(jnp.abs(master_down), axis=2),
        ),
        "zero",
    )
    narrow_gate, narrow_up, narrow_down = (
        (master_gate / jnp.expand_dims(scale_gate, 1)).astype(jnp.bfloat16),
        (master_up / jnp.expand_dims(scale_up, 1)).astype(jnp.bfloat16),
        (master_down / jnp.expand_dims(scale_down, 2)).astype(jnp.bfloat16),
    )
    final_gate, final_up = (
        lax.all_to_all(narrow_gate, "zero", split_axis=2, concat_axis=1, tiled=True),
        lax.all_to_all(narrow_up, "zero", split_axis=2, concat_axis=1, tiled=True),
    )
    final_down = lax.all_to_all(narrow_down, "zero", split_axis=1, concat_axis=2, tiled=True)
    scale_gate = lax.dynamic_slice_in_dim(
        scale_gate, lax.axis_index("zero") * final_gate.shape[2], final_gate.shape[2], axis=1
    )
    scale_up = lax.dynamic_slice_in_dim(
        scale_up, lax.axis_index("zero") * final_up.shape[2], final_up.shape[2], axis=1
    )
    scale_down = lax.dynamic_slice_in_dim(
        scale_down, lax.axis_index("zero") * final_down.shape[1], final_down.shape[1], axis=1
    )
    part_router = (router_weight * router_gain[:, None]).astype(jnp.bfloat16)
    row_router = lax.all_gather(part_router, "zero", axis=0, tiled=True)
    serve_router = lax.all_gather(row_router, "bank", axis=1, tiled=True)
    return (final_gate, final_up, final_down, scale_gate, scale_up, scale_down, serve_router)


def exchange_kernel(
    n, banks, first, late,
    gate, up, down, router, gain,
    out_gate, out_up, out_down, *rest,
):
    out_lates, rest = rest[: n // 2], rest[n // 2 :]
    exchange_body(n, banks, first, late, gate, up, down, router, gain, out_gate, out_up, out_down, out_lates, *rest)


def exchange_body(
    n, banks, first, late,
    gate, up, down, router, gain,
    out_gate, out_up, out_down, out_lates, out_scale, out_router,
    mrow, mcol, srow, scol, slots, latebuf, partial, direct, scale, rw, rg, rt, half_a, half_b,
    mload_sem, sload_sem, send_sem, local_sem, late_sem, late_send, late_recv, recv_sem,
    dx_send, dx_recv, hx_send, hx_recv, r0_sem, r1_send, r1_recv, r2_send, r2_recv,
):
    me = lax.axis_index("zero")
    bank = lax.axis_index("bank")
    experts, rows, width = gate.shape
    piece = width // n
    levels = len(half_a)
    nx, ns = mrow.shape[0], slots.shape[0]
    sources, outs = (gate, up, down), (out_gate, out_up, out_down)
    cols = router.shape[0]

    def peer(k):
        return lax.rem(me + k, n)

    def bank_peer(k):
        return lax.rem(bank + k, banks)

    def load(bufs, sem, m, e):
        b = lax.rem(e, nx)
        return pltpu.make_async_copy(sources[m].at[e], bufs[m].at[b], sem.at[m // 2, b])

    def prime(bufs, sem, m, lo, hi):
        for i in range(min(nx - 1, hi - lo)):
            load(bufs, sem, m, lo + i).start()

    def stream(bufs, sem, m, lo, hi, end, body):
        def step(e, _):
            @pl.when(e + nx - 1 < end)
            def _():
                load(bufs, sem, m, e + nx - 1).start()

            body(e, bufs[m].at[lax.rem(e, nx)], load(bufs, sem, m, e))
            return 0

        lax.fori_loop(lo, hi, step, 0)

    mbufs, sbufs = (mrow, mrow, mcol), (srow, srow, scol)

    def maxima(m, lo, hi, end):
        def body(e, x, arrival):
            arrival.wait()
            u = m * experts + e
            if m < 2:
                partial[u] = jnp.max(jnp.abs(x[...]), axis=0, keepdims=True)
            else:
                top = jnp.abs(x[:, :LANES])
                for j in range(1, rows // LANES):
                    top = jnp.maximum(top, jnp.abs(x[:, j * LANES : (j + 1) * LANES]))
                partial[u] = jnp.max(top.T, axis=0, keepdims=True)

        stream(mbufs, mload_sem, m, lo, hi, end, body)

    def dx(b, lo, hi, k):
        return pltpu.make_async_remote_copy(
            src_ref=partial.at[pl.ds(lo, hi - lo)],
            dst_ref=direct.at[k - 1, pl.ds(lo, hi - lo)],
            send_sem=dx_send.at[b, k - 1],
            recv_sem=dx_recv.at[b, k - 1],
            device_id=(bank, peer(k)),
            device_id_type=MESH,
        )

    def dx_start(b, lo, hi):
        for k in range(1, n):
            dx(b, lo, hi, k).start()

    def dx_finish(b, lo, hi):
        for k in range(1, n):
            dx(b, lo, hi, k).wait()
        top = partial[pl.ds(lo, hi - lo)]
        for k in range(1, n):
            top = jnp.maximum(top, direct[k - 1, pl.ds(lo, hi - lo)])
        scale[pl.ds(lo, hi - lo)] = top

    def hx_ranges(lo, size):
        start, out = lo, []
        for i in range(levels - 1):
            part = size // 2
            bit = lax.rem(me // (1 << i), 2)
            out.append((start + bit * part, start + (1 - bit) * part, part))
            start, size = start + bit * part, part
        return out, start, size

    def hx(b, lo, size, stage):
        bufs = (half_a, half_b)[b]
        ranges, start, part = hx_ranges(lo, size)
        if stage < levels - 1:
            level = stage
            src, dst = partial.at[pl.ds(ranges[level][1], ranges[level][2])], bufs[level]
        elif stage == levels - 1:
            level = stage
            src, dst = partial.at[pl.ds(start, part)], bufs[level]
        else:
            level = 2 * (levels - 1) - stage
            src = scale.at[pl.ds(ranges[level][0], ranges[level][2])]
            dst = src
        bit = lax.rem(me // (1 << level), 2)
        return pltpu.make_async_remote_copy(
            src_ref=src,
            dst_ref=dst,
            send_sem=hx_send.at[b, stage],
            recv_sem=hx_recv.at[b, stage],
            device_id=(bank, me + (1 - 2 * bit) * (1 << level)),
            device_id_type=MESH,
        )

    def hx_start(b, lo, size, stage):
        hx(b, lo, size, stage).start()

    def hx_finish(b, lo, size, stage):
        bufs = (half_a, half_b)[b]
        hx(b, lo, size, stage).wait()
        ranges, start, part = hx_ranges(lo, size)
        if stage < levels - 1:
            keep = pl.ds(ranges[stage][0], ranges[stage][2])
            partial[keep] = jnp.maximum(partial[keep], bufs[stage][...])
        elif stage == levels - 1:
            scale[pl.ds(start, part)] = jnp.maximum(partial[pl.ds(start, part)], bufs[stage][...])

    def bulk(m, e, s, k):
        p = peer(k)
        return pltpu.make_async_remote_copy(
            src_ref=slots.at[s, pl.ds(pl.multiple_of(p * piece, 16), piece)],
            dst_ref=outs[m].at[e, :, pl.ds(pl.multiple_of(me * rows, LANES), rows)],
            send_sem=send_sem.at[s, k - 1],
            recv_sem=recv_sem.at[m, k - 1],
            device_id=(bank, p),
            device_id_type=MESH,
        )

    def own(m, e, s):
        return pltpu.make_async_copy(
            slots.at[s, pl.ds(pl.multiple_of(me * piece, 16), piece)],
            outs[m].at[e, :, pl.ds(pl.multiple_of(me * rows, LANES), rows)],
            local_sem.at[s],
        )

    def free(s):
        for k in range(1, n):
            bulk(0, 0, s, k).wait_send()
        own(0, 0, s).wait()

    def narrow(m, e, x, out):
        top = scale[m * experts + e]
        for j in range(width // LANES):
            cut = slice(j * LANES, (j + 1) * LANES)
            if m < 2:
                out[cut, :] = (x[:, cut] / top[:, cut]).T.astype(jnp.bfloat16)
            else:
                col = jnp.broadcast_to(top[:, cut], (LANES, LANES)).T
                for i in range(rows // LANES):
                    lane = slice(i * LANES, (i + 1) * LANES)
                    out[cut, lane] = (x[cut, lane] / col).astype(jnp.bfloat16)

    def send(m, lo, hi, before=None, after=None):
        def body(e, x, arrival):
            g = m * experts + e
            s = lax.rem(g, ns)

            @pl.when(g >= ns)
            def _():
                free(s)

            if before:
                before(e)
            arrival.wait()
            narrow(m, e, x, slots.at[s])
            for k in range(1, n):
                bulk(m, e, s, k).start()
            own(m, e, s).start()
            if after:
                after(e)

        stream(sbufs, sload_sem, m, lo, hi, hi, body)

    def r1(k):
        mine = rt.at[pl.ds(pl.multiple_of(bank * cols, 16), cols), pl.ds(pl.multiple_of(me * rows, LANES), rows)]
        return pltpu.make_async_remote_copy(
            src_ref=mine, dst_ref=mine, send_sem=r1_send.at[k - 1], recv_sem=r1_recv.at[k - 1],
            device_id=(bank, peer(k)), device_id_type=MESH,
        )

    def r2(k):
        mine = rt.at[pl.ds(pl.multiple_of(bank * cols, 16), cols)]
        return pltpu.make_async_remote_copy(
            src_ref=mine, dst_ref=mine, send_sem=r2_send.at[k - 1], recv_sem=r2_recv.at[k - 1],
            device_id=(bank_peer(k), me), device_id_type=MESH,
        )

    def r0():
        return pltpu.make_async_copy(router, rw, r0_sem.at[0]), pltpu.make_async_copy(gain, rg, r0_sem.at[1])

    prime(mbufs, mload_sem, 0, 0, experts)
    for copy in r0():
        copy.start()
    barrier = pltpu.get_barrier_semaphore()
    for k in range(1, n):
        pl.semaphore_signal(barrier, inc=1, device_id=(bank, peer(k)), device_id_type=MESH)
    for k in range(1, banks):
        pl.semaphore_signal(barrier, inc=1, device_id=(bank_peer(k), me), device_id_type=MESH)
    maxima(0, 0, 1, experts)
    pl.semaphore_wait(barrier, n - 1 + banks - 1)
    dx_start(0, 0, 1)
    prime(sbufs, sload_sem, 0, 0, experts)
    maxima(0, 1, first, experts)
    dx_start(1, 1, first)
    for copy in r0():
        copy.wait()
    rt[pl.ds(pl.multiple_of(bank * cols, 16), cols), pl.ds(pl.multiple_of(me * rows, LANES), rows)] = (
        rw[...] * rg[...]
    ).astype(jnp.bfloat16)
    for k in range(1, n):
        r1(k).start()
    dx_finish(0, 0, 1)

    batches = ((0, first, experts - first), (1, experts, 2 * experts))
    last = 2 * (levels - 1)

    def before(e):
        @pl.when(e == 1)
        def _():
            maxima(0, first, experts, experts)
            dx_finish(1, 1, first)
            hx_start(*batches[0], 0)
            hx_finish(*batches[0], 0)
            hx_start(*batches[0], 1)

        for stage in range(1, last):
            @pl.when(e == stage + 1)
            def _():
                hx_finish(*batches[0], stage)
                hx_start(*batches[0], stage + 1)
                if stage == last - 1:
                    hx_finish(*batches[0], last)

        @pl.when(e == first + 1)
        def _():
            for k in range(1, n):
                r1(k).wait()
            for k in range(1, banks):
                r2(k).start()

        for stage in range(last):
            @pl.when(e == 2 * (first + stage))
            def _():
                hx_finish(*batches[1], stage)
                hx_start(*batches[1], stage + 1)

        @pl.when(e == 2 * (first + last) - 1)
        def _():
            hx_finish(*batches[1], last)

    def after(e):
        for i in range(4):
            @pl.when(e == first + i)
            def _():
                m, lo = 1 + i // 2, (i % 2) * (experts // 2)
                hi = lo + experts // 2
                prime(mbufs, mload_sem, m, lo, hi)
                maxima(m, lo, hi, hi)

        @pl.when(e == first + 3)
        def _():
            hx_start(*batches[1], 0)

    send(0, 0, experts, before, after)
    prime(sbufs, sload_sem, 1, 0, experts)
    send(1, 0, experts)
    out_scale[...] = scale[...]

    half = n // 2
    mine = pl.ds(pl.multiple_of(me * rows, LANES), rows)

    def flip(k):
        return me + sum((1 - 2 * lax.rem(me // (1 << i), 2)) * (k & (1 << i)) for i in range(levels))

    def cut_of(t, p):
        return latebuf.at[t, pl.ds(pl.multiple_of(p * piece, 16), piece)]

    def late_keep(t, j):
        return pltpu.make_async_copy(cut_of(t, flip(half + j)), out_lates[j].at[t], late_sem.at[t, j])

    def late_own(t, e):
        return pltpu.make_async_copy(cut_of(t, me), out_down.at[e, :, mine], late_sem.at[t, half])

    def late_near(t, e, k):
        return pltpu.make_async_remote_copy(
            src_ref=cut_of(t, flip(k)),
            dst_ref=out_down.at[e, :, mine],
            send_sem=late_send.at[t, k - 1],
            recv_sem=late_recv.at[k - 1],
            device_id=(bank, flip(k)),
            device_id_type=MESH,
        )

    def stage_late(e, x, arrival):
        arrival.wait()
        t = e - (experts - late)
        narrow(2, e, x, latebuf.at[t])
        for k in range(1, half):
            late_near(t, e, k).start()
        late_own(t, e).start()
        for j in range(half):
            late_keep(t, j).start()

    prime(sbufs, sload_sem, 2, experts - late, experts)
    stream(sbufs, sload_sem, 2, experts - late, experts, experts, stage_late)
    prime(sbufs, sload_sem, 2, 0, experts - late)
    send(2, 0, experts - late)
    for k in range(1, banks):
        r2(k).wait()
    out_router[...] = rt[...]
    for t in range(late):
        for k in range(1, half):
            late_near(t, 0, k).wait_send()
        late_own(t, 0).wait()
        for j in range(half):
            late_keep(t, j).wait()
    for k in range(1, half):
        whole = out_down.at[pl.ds(0, late), :, pl.ds(0, rows)]
        pltpu.make_async_copy(whole, whole, late_recv.at[k - 1]).wait()
    for s in range(ns):
        free(s)
    for m in range(3):
        count = experts - late if m == 2 else experts
        for k in range(1, n):
            whole = outs[m].at[pl.ds(0, count), :, pl.ds(0, rows)]
            pltpu.make_async_copy(whole, whole, recv_sem.at[m, k - 1]).wait()


def place_kernel(
    n, late, gate, up, down, router, out_gate, out_up, out_down, out_router, ring, in_sem, out_sem, router_sem
):
    experts, depth = gate.shape[0], ring.shape[0]
    half = gate.shape[2] // 2
    near = pl.ds(pl.multiple_of(lax.axis_index("zero") // (n // 2) * half, LANES), half)
    pairs = ((gate, out_gate), (up, out_up), (down, out_down))
    blocks = [(m, e) for m in range(3) for e in range(experts)]

    def views(i):
        m, e = blocks[i]
        if m == 2 and e >= experts - late:
            return pairs[m][0].at[e, :, near], ring.at[i % depth, :, pl.ds(0, half)], pairs[m][1].at[e, :, near]
        return pairs[m][0].at[e], ring.at[i % depth], pairs[m][1].at[e]

    def take(i):
        source, hold, _ = views(i)
        return pltpu.make_async_copy(source, hold, in_sem.at[i % depth])

    def put(i):
        _, hold, target = views(i)
        return pltpu.make_async_copy(hold, target, out_sem.at[i % depth])

    whole_router = pltpu.make_async_copy(router, out_router, router_sem)
    whole_router.start()
    lead = depth // 2
    for i in range(len(blocks) + lead):
        if i < len(blocks):
            if i >= depth:
                put(i - depth).wait()
            take(i).start()
        if i >= lead:
            take(i - lead).wait()
            put(i - lead).start()
    for i in range(max(0, len(blocks) - depth), len(blocks)):
        put(i).wait()
    whole_router.wait()


def late_kernel(*refs):
    *got, down, out, out_sem = refs
    half = len(got)
    late, _, rows = got[0].shape
    experts = down.shape[0]
    me = lax.axis_index("zero")

    def put(j):
        k = half + j
        bits = [i for i in range(k.bit_length()) if k & (1 << i)]
        p = me + sum((1 - 2 * lax.rem(me // (1 << i), 2)) * (1 << i) for i in bits)
        lanes = pl.ds(pl.multiple_of(p * rows, LANES), rows)
        return pltpu.make_async_copy(got[j], out.at[pl.ds(experts - late, late), :, lanes], out_sem.at[j])

    for j in range(half):
        put(j).start()
    for j in range(half):
        put(j).wait()


def fused_shards(n, banks, master_gate, master_up, master_down, router_weight, router_gain):
    experts, rows, width = master_gate.shape
    piece = width // n
    columns = router_weight.shape[1]
    units, first, late, half = 3 * experts, n // 2, LATE, n // 2
    levels = n.bit_length() - 1
    final = jax.ShapeDtypeStruct((experts, piece, n * rows), jnp.bfloat16)
    hbm, vmem = pl.BlockSpec(memory_space=pl.ANY), pl.BlockSpec(memory_space=pltpu.VMEM)
    dma = pltpu.SemaphoreType.DMA
    nx, ns = 4, SLOTS

    def halves(size):
        return tuple(
            pltpu.VMEM((size >> min(i + 1, levels - 1), 1, width), jnp.float32) for i in range(levels)
        )

    gate, up, down, *tails, scale, router = pl.pallas_call(
        functools.partial(exchange_kernel, n, banks, first, late),
        out_shape=[
            final,
            final,
            final,
            *[jax.ShapeDtypeStruct((late, piece, rows), jnp.bfloat16)] * half,
            jax.ShapeDtypeStruct((units, 1, width), jnp.float32),
            jax.ShapeDtypeStruct((banks * columns, n * rows), jnp.bfloat16),
        ],
        in_specs=[hbm] * 5,
        out_specs=[hbm] * (3 + half) + [vmem, vmem],
        scratch_shapes=[
            pltpu.VMEM((nx, rows, width), jnp.float32),
            pltpu.VMEM((nx, width, rows), jnp.float32),
            pltpu.VMEM((nx, rows, width), jnp.float32),
            pltpu.VMEM((nx, width, rows), jnp.float32),
            pltpu.VMEM((ns, width, rows), jnp.bfloat16),
            pltpu.VMEM((late, width, rows), jnp.bfloat16),
            pltpu.VMEM((units, 1, width), jnp.float32),
            pltpu.VMEM((n - 1, first, 1, width), jnp.float32),
            pltpu.VMEM((units, 1, width), jnp.float32),
            pltpu.VMEM((columns, rows), jnp.float32),
            pltpu.VMEM((1, rows), jnp.float32),
            pltpu.VMEM((banks * columns, n * rows), jnp.bfloat16),
            halves(experts - first),
            halves(2 * experts),
            dma((2, nx)),
            dma((2, nx)),
            dma((ns, n - 1)),
            dma((ns,)),
            dma((late, half + 1)),
            dma((late, half - 1)),
            dma((half - 1,)),
            dma((3, n - 1)),
            dma((2, n - 1)),
            dma((2, n - 1)),
            dma((2, 2 * levels - 1)),
            dma((2, 2 * levels - 1)),
            dma((2,)),
            dma((n - 1,)),
            dma((n - 1,)),
            dma((banks - 1,)),
            dma((banks - 1,)),
        ],
        compiler_params=pltpu.CompilerParams(
            collective_id=0, has_side_effects=True, vmem_limit_bytes=56 * 1024 * 1024
        ),
    )(master_gate, master_up, master_down, router_weight.T, router_gain[None, :])
    got = [None] * half
    for j in reversed(range(half)):
        got[j] = lax.ppermute(tails[j], "zero", [(i, i ^ (half + j)) for i in range(n)])
    depth = 16
    moved = 2 * 2 * (3 * experts - late) * piece * n * rows
    final_gate, final_up, final_down, router = pl.pallas_call(
        functools.partial(place_kernel, n, late),
        out_shape=[final, final, final, jax.ShapeDtypeStruct(router.shape, router.dtype)],
        in_specs=[hbm] * 3 + [vmem],
        out_specs=[hbm] * 4,
        scratch_shapes=[
            pltpu.VMEM((depth, piece, n * rows), jnp.bfloat16),
            dma((depth,)),
            dma((depth,)),
            dma,
        ],
        compiler_params=pltpu.CompilerParams(vmem_limit_bytes=56 * 1024 * 1024),
        cost_estimate=pl.CostEstimate(flops=0, bytes_accessed=moved, transcendentals=0),
    )(gate, up, down, router)
    final_down = pl.pallas_call(
        late_kernel,
        out_shape=final,
        in_specs=[vmem] * half + [hbm],
        out_specs=hbm,
        input_output_aliases={half: 0},
        scratch_shapes=[dma((half,))],
        compiler_params=pltpu.CompilerParams(vmem_limit_bytes=8 * 1024 * 1024),
        cost_estimate=pl.CostEstimate(
            flops=0, bytes_accessed=4 * late * piece * n * rows, transcendentals=0
        ),
    )(*got, final_down)
    mine = lax.dynamic_slice_in_dim(
        scale.reshape(3, experts, width), lax.axis_index("zero") * piece, piece, axis=2
    )
    return (
        jnp.swapaxes(final_gate, 1, 2),
        jnp.swapaxes(final_up, 1, 2),
        final_down,
        mine[0],
        mine[1],
        mine[2],
        router.T,
    )


def shards(n, banks, *arrays):
    experts, rows, width = arrays[0].shape
    fits = (
        experts % n == 0
        and experts >= 2 * n
        and n == 1 << (n.bit_length() - 1)
        and rows % LANES == 0
        and width % LANES == 0
        and width // n % 16 == 0
        and arrays[3].shape[1] % 16 == 0
        and n == 8
        and banks > 1
    )
    return fused_shards(n, banks, *arrays) if fits else plain_shards(*arrays)


def solution(mesh):
    placed = (
        P("bank", "zero", None),
        P("bank", "zero", None),
        P("bank", None, "zero"),
        P("zero", "bank"),
        P("zero"),
    )
    return jax.shard_map(
        functools.partial(shards, mesh.shape["zero"], mesh.shape["bank"]),
        mesh=mesh,
        in_specs=placed,
        out_specs=(
            P("bank", None, "zero"),
            P("bank", None, "zero"),
            P("bank", "zero", None),
            P("bank", "zero"),
            P("bank", "zero"),
            P("bank", "zero"),
            P(),
        ),
        check_vma=False,
    )
```

```python
import functools

import jax
import jax.numpy as jnp
from jax import lax
from jax.experimental import pallas as pl
from jax.experimental.pallas import tpu as pltpu
from jax.sharding import PartitionSpec as P

MESH = pl.DeviceIdType.MESH
LANES = 128
LATE = 3
AHEAD = 8
EARLY = 4
SLOTS = 3


def plain_shards(master_gate, master_up, master_down, router_weight, router_gain):
    scale_gate, scale_up, scale_down = lax.pmax(
        (
            jnp.max(jnp.abs(master_gate), axis=1),
            jnp.max(jnp.abs(master_up), axis=1),
            jnp.max(jnp.abs(master_down), axis=2),
        ),
        "zero",
    )
    narrow_gate, narrow_up, narrow_down = (
        (master_gate / jnp.expand_dims(scale_gate, 1)).astype(jnp.bfloat16),
        (master_up / jnp.expand_dims(scale_up, 1)).astype(jnp.bfloat16),
        (master_down / jnp.expand_dims(scale_down, 2)).astype(jnp.bfloat16),
    )
    final_gate, final_up = (
        lax.all_to_all(narrow_gate, "zero", split_axis=2, concat_axis=1, tiled=True),
        lax.all_to_all(narrow_up, "zero", split_axis=2, concat_axis=1, tiled=True),
    )
    final_down = lax.all_to_all(narrow_down, "zero", split_axis=1, concat_axis=2, tiled=True)
    scale_gate = lax.dynamic_slice_in_dim(
        scale_gate, lax.axis_index("zero") * final_gate.shape[2], final_gate.shape[2], axis=1
    )
    scale_up = lax.dynamic_slice_in_dim(
        scale_up, lax.axis_index("zero") * final_up.shape[2], final_up.shape[2], axis=1
    )
    scale_down = lax.dynamic_slice_in_dim(
        scale_down, lax.axis_index("zero") * final_down.shape[1], final_down.shape[1], axis=1
    )
    part_router = (router_weight * router_gain[:, None]).astype(jnp.bfloat16)
    row_router = lax.all_gather(part_router, "zero", axis=0, tiled=True)
    serve_router = lax.all_gather(row_router, "bank", axis=1, tiled=True)
    return (final_gate, final_up, final_down, scale_gate, scale_up, scale_down, serve_router)


def exchange_kernel(
    n, banks, first, late, ahead,
    gate, up, down, router, gain,
    out_gate, out_up, out_down, *rest,
):
    out_lates, rest = rest[: n // 2], rest[n // 2 :]
    exchange_body(n, banks, first, late, ahead, gate, up, down, router, gain, out_gate, out_up, out_down, out_lates, *rest)


def exchange_body(
    n, banks, first, late, ahead,
    gate, up, down, router, gain,
    out_gate, out_up, out_down, out_lates, out_scale, out_router,
    mrow, mcol, srow, scol, slots, early, partial, direct, pair_in, pair, pairs_in, quick, scale, rw, rg, rt, half_a, half_b,
    mload_sem, sload_sem, send_sem, local_sem, early_sem, early_send, early_recv, recv_sem,
    dx_send, dx_recv, q_send, q_recv, hx_send, hx_recv, r0_sem, r1_send, r1_recv, rx_send, rx_recv, r2_send, r2_recv,
):
    me = lax.axis_index("zero")
    bank = lax.axis_index("bank")
    experts, rows, width = gate.shape
    piece = width // n
    levels = len(half_a)
    nx, ns = mrow.shape[0], slots.shape[0]
    sources, outs = (gate, up, down), (out_gate, out_up, out_down)
    cols = router.shape[0]

    half = n // 2
    mine = pl.ds(pl.multiple_of(me * rows, LANES), rows)

    def flip(k):
        return me + sum((1 - 2 * lax.rem(me // (1 << i), 2)) * (k & (1 << i)) for i in range(levels))

    def bank_peer(k):
        return lax.rem(bank + k, banks)

    def load(bufs, sem, m, e):
        b = lax.rem(e, nx)
        return pltpu.make_async_copy(sources[m].at[e], bufs[m].at[b], sem.at[m // 2, b])

    def prime(bufs, sem, m, lo, hi):
        for i in range(min(nx - 1, hi - lo)):
            load(bufs, sem, m, lo + i).start()

    def stream(bufs, sem, m, lo, hi, end, body):
        def step(e, _):
            @pl.when(e + nx - 1 < end)
            def _():
                load(bufs, sem, m, e + nx - 1).start()

            body(e, bufs[m].at[lax.rem(e, nx)], load(bufs, sem, m, e))
            return 0

        lax.fori_loop(lo, hi, step, 0)

    mbufs, sbufs = (mrow, mrow, mcol), (srow, srow, scol)

    def maxima(m, lo, hi, end):
        def body(e, x, arrival):
            arrival.wait()
            u = m * experts + e
            if m < 2:
                partial[u] = jnp.max(jnp.abs(x[...]), axis=0, keepdims=True)
            else:
                top = jnp.abs(x[:, :LANES])
                for j in range(1, rows // LANES):
                    top = jnp.maximum(top, jnp.abs(x[:, j * LANES : (j + 1) * LANES]))
                partial[u] = jnp.max(top.T, axis=0, keepdims=True)

        stream(mbufs, mload_sem, m, lo, hi, end, body)

    def dx(k):
        return pltpu.make_async_remote_copy(
            src_ref=partial.at[0],
            dst_ref=direct.at[k - 1],
            send_sem=dx_send.at[k - 1],
            recv_sem=dx_recv.at[k - 1],
            device_id=(bank, flip(k)),
            device_id_type=MESH,
        )

    def dx_finish():
        top = partial[0]
        for k in range(1, n):
            dx(k).wait()
            top = jnp.maximum(top, direct[k - 1])
        scale[0] = top

    share = first // 2
    side = lax.rem(me, 2)
    ours = pl.ds(side * share, share)

    def qa():
        return pltpu.make_async_remote_copy(
            src_ref=partial.at[pl.ds((1 - side) * share, share)],
            dst_ref=pair_in,
            send_sem=q_send.at[0],
            recv_sem=q_recv.at[0],
            device_id=(bank, flip(1)),
            device_id_type=MESH,
        )

    def qb(i):
        return pltpu.make_async_remote_copy(
            src_ref=pair,
            dst_ref=pairs_in.at[i - 1],
            send_sem=q_send.at[i],
            recv_sem=q_recv.at[i],
            device_id=(bank, flip(2 * i)),
            device_id_type=MESH,
        )

    def qc():
        return pltpu.make_async_remote_copy(
            src_ref=quick.at[ours],
            dst_ref=quick.at[ours],
            send_sem=q_send.at[half],
            recv_sem=q_recv.at[half],
            device_id=(bank, flip(1)),
            device_id_type=MESH,
        )

    def quick_start():
        qa().wait()
        pair[...] = jnp.maximum(partial[ours], pair_in[...])
        for i in range(1, half):
            qb(i).start()

    def quick_finish():
        top = pair[...]
        for i in range(1, half):
            qb(i).wait()
            top = jnp.maximum(top, pairs_in[i - 1])
        quick[ours] = top
        qc().start()
        qc().wait()
        scale[pl.ds(1, first - 1)] = quick[pl.ds(1, first - 1)]

    def hx_ranges(lo, size):
        start, out = lo, []
        for i in range(levels - 1):
            part = size // 2
            bit = lax.rem(me // (1 << i), 2)
            out.append((start + bit * part, start + (1 - bit) * part, part))
            start, size = start + bit * part, part
        return out, start, size

    def hx(b, lo, size, stage):
        bufs = (half_a, half_b)[b]
        ranges, start, part = hx_ranges(lo, size)
        if stage < levels - 1:
            level = stage
            src, dst = partial.at[pl.ds(ranges[level][1], ranges[level][2])], bufs[level]
        elif stage == levels - 1:
            level = stage
            src, dst = partial.at[pl.ds(start, part)], bufs[level]
        else:
            level = 2 * (levels - 1) - stage
            src = scale.at[pl.ds(ranges[level][0], ranges[level][2])]
            dst = src
        bit = lax.rem(me // (1 << level), 2)
        return pltpu.make_async_remote_copy(
            src_ref=src,
            dst_ref=dst,
            send_sem=hx_send.at[b, stage],
            recv_sem=hx_recv.at[b, stage],
            device_id=(bank, me + (1 - 2 * bit) * (1 << level)),
            device_id_type=MESH,
        )

    def hx_start(b, lo, size, stage):
        hx(b, lo, size, stage).start()

    def hx_finish(b, lo, size, stage):
        bufs = (half_a, half_b)[b]
        hx(b, lo, size, stage).wait()
        ranges, start, part = hx_ranges(lo, size)
        if stage < levels - 1:
            keep = pl.ds(ranges[stage][0], ranges[stage][2])
            partial[keep] = jnp.maximum(partial[keep], bufs[stage][...])
        elif stage == levels - 1:
            scale[pl.ds(start, part)] = jnp.maximum(partial[pl.ds(start, part)], bufs[stage][...])

    def bulk(m, e, s, k):
        p = flip(k)
        return pltpu.make_async_remote_copy(
            src_ref=slots.at[s, pl.ds(pl.multiple_of(p * piece, 16), piece)],
            dst_ref=outs[m].at[e, :, pl.ds(pl.multiple_of(me * rows, LANES), rows)],
            send_sem=send_sem.at[s, k - 1],
            recv_sem=recv_sem.at[m, k - 1],
            device_id=(bank, p),
            device_id_type=MESH,
        )

    def own(m, e, s):
        return pltpu.make_async_copy(
            slots.at[s, pl.ds(pl.multiple_of(me * piece, 16), piece)],
            outs[m].at[e, :, pl.ds(pl.multiple_of(me * rows, LANES), rows)],
            local_sem.at[s],
        )

    def free(s, low=1):
        for k in range(low, n):
            bulk(0, 0, s, k).wait_send()
        if low == 1:
            own(0, 0, s).wait()

    def narrow(m, e, x, out):
        top = scale[m * experts + e]
        for j in range(width // LANES):
            cut = slice(j * LANES, (j + 1) * LANES)
            if m < 2:
                out[cut, :] = (x[:, cut] / top[:, cut]).T.astype(jnp.bfloat16)
            else:
                col = jnp.broadcast_to(top[:, cut], (LANES, LANES)).T
                for i in range(rows // LANES):
                    lane = slice(i * LANES, (i + 1) * LANES)
                    out[cut, lane] = (x[cut, lane] / col).astype(jnp.bfloat16)

    turn = 2 * experts + experts - ahead

    def send(m, lo, hi, before=None, after=None, low=1):
        def body(e, x, arrival):
            g = m * experts + e
            s = lax.rem(g, ns)

            @pl.when((g >= ns) & (g - ns < turn))
            def _():
                free(s)

            @pl.when(g - ns >= turn)
            def _():
                free(s, half)

            if before:
                before(e)
            arrival.wait()
            narrow(m, e, x, slots.at[s])
            for k in range(low, n):
                bulk(m, e, s, k).start()
            if low == 1:
                own(m, e, s).start()
            if after:
                after(e)

        stream(sbufs, sload_sem, m, lo, hi, hi, body)

    def route(q):
        return rt.at[pl.ds(pl.multiple_of(bank * cols, 16), cols), pl.ds(pl.multiple_of(q * rows, LANES), rows)]

    def r1(i):
        return pltpu.make_async_remote_copy(
            src_ref=route(me), dst_ref=route(me), send_sem=r1_send.at[i - 1], recv_sem=r1_recv.at[i - 1],
            device_id=(bank, flip(2 * i)), device_id_type=MESH,
        )

    def rx(i):
        q = flip(2 * i)
        return pltpu.make_async_remote_copy(
            src_ref=route(q), dst_ref=route(q), send_sem=rx_send.at[i], recv_sem=rx_recv.at[i],
            device_id=(bank, flip(1)), device_id_type=MESH,
        )

    def r2(k):
        mine = rt.at[pl.ds(pl.multiple_of(bank * cols, 16), cols)]
        return pltpu.make_async_remote_copy(
            src_ref=mine, dst_ref=mine, send_sem=r2_send.at[k - 1], recv_sem=r2_recv.at[k - 1],
            device_id=(bank_peer(k), me), device_id_type=MESH,
        )

    def r0():
        return pltpu.make_async_copy(router, rw, r0_sem.at[0]), pltpu.make_async_copy(gain, rg, r0_sem.at[1])

    prime(mbufs, mload_sem, 0, 0, experts)
    for copy in r0():
        copy.start()
    barrier = pltpu.get_barrier_semaphore()
    for k in range(1, n):
        pl.semaphore_signal(barrier, inc=1, device_id=(bank, flip(k)), device_id_type=MESH)
    for k in range(1, banks):
        pl.semaphore_signal(barrier, inc=1, device_id=(bank_peer(k), me), device_id_type=MESH)
    maxima(0, 0, 1, experts)
    for copy in r0():
        copy.wait()
    rt[pl.ds(pl.multiple_of(bank * cols, 16), cols), pl.ds(pl.multiple_of(me * rows, LANES), rows)] = (
        rw[...] * rg[...]
    ).astype(jnp.bfloat16)
    pl.semaphore_wait(barrier, n - 1 + banks - 1)
    for k in range(1, n):
        dx(k).start()
    for i in range(1, half):
        r1(i).start()
    prime(sbufs, sload_sem, 0, 0, experts)
    maxima(0, 1, first, experts)
    qa().start()
    quick_start()
    dx_finish()

    batches = ((0, first, experts - first), (1, experts, 2 * experts))
    last = 2 * (levels - 1)

    def before(e):
        @pl.when(e == 1)
        def _():
            maxima(0, first, experts, experts)
            quick_finish()
            hx_start(*batches[0], 0)
            hx_finish(*batches[0], 0)
            hx_start(*batches[0], 1)

        for stage in range(1, last):
            @pl.when(e == stage + 1)
            def _():
                hx_finish(*batches[0], stage)
                hx_start(*batches[0], stage + 1)
                if stage == last - 1:
                    hx_finish(*batches[0], last)

        @pl.when(e == first)
        def _():
            for i in range(1, half):
                r1(i).wait()
            for i in range(half):
                rx(i).start()

        @pl.when(e == first + 2)
        def _():
            for i in range(half):
                rx(i).wait()
            for k in range(1, banks):
                r2(k).start()

        for stage in range(last):
            @pl.when(e == 2 * (first + stage))
            def _():
                hx_finish(*batches[1], stage)
                hx_start(*batches[1], stage + 1)

        @pl.when(e == 2 * (first + last) - 1)
        def _():
            hx_finish(*batches[1], last)

    def after(e):
        for i in range(4):
            @pl.when(e == first + i)
            def _():
                m, lo = 1 + i // 2, (i % 2) * (experts // 2)
                hi = lo + experts // 2
                prime(mbufs, mload_sem, m, lo, hi)
                maxima(m, lo, hi, hi)

        @pl.when(e == first + 3)
        def _():
            hx_start(*batches[1], 0)

    send(0, 0, experts, before, after)
    prime(sbufs, sload_sem, 1, 0, experts)
    prime(sbufs, sload_sem, 2, experts - ahead, experts)

    def cut_of(b, p):
        return early.at[b, pl.ds(pl.multiple_of(p * piece, 16), piece)]

    def early_keep(b, t, j):
        return pltpu.make_async_copy(cut_of(b, flip(half + j)), out_lates[j].at[t], early_sem.at[b, j])

    def early_own(b, e):
        return pltpu.make_async_copy(cut_of(b, me), out_down.at[e, :, mine], early_sem.at[b, half])

    def early_near(b, e, k):
        return pltpu.make_async_remote_copy(
            src_ref=cut_of(b, flip(k)),
            dst_ref=out_down.at[e, :, mine],
            send_sem=early_send.at[b, k - 1],
            recv_sem=early_recv.at[k - 1],
            device_id=(bank, flip(k)),
            device_id_type=MESH,
        )

    def early_free(b):
        for k in range(1, half):
            early_near(b, 0, k).wait_send()
        early_own(b, 0).wait()

    def go_early(up_e):
        step = experts // ahead

        @pl.when(lax.rem(up_e, step) == step - 1)
        def _():
            i = up_e // step
            e = experts - ahead + i
            b = lax.rem(i, EARLY)

            @pl.when(i >= EARLY)
            def _():
                early_free(b)

            @pl.when(e + nx - 1 < experts)
            def _():
                load(sbufs, sload_sem, 2, e + nx - 1).start()

            load(sbufs, sload_sem, 2, e).wait()
            narrow(2, e, scol.at[lax.rem(e, nx)], early.at[b])
            for k in range(1, half):
                early_near(b, e, k).start()
            early_own(b, e).start()

            @pl.when(e >= experts - late)
            def _():
                for j in range(half):
                    early_keep(b, e - (experts - late), j).start()

    send(1, 0, experts, after=go_early)
    out_scale[...] = scale[...]
    prime(sbufs, sload_sem, 2, 0, experts - ahead)
    send(2, 0, experts - ahead)
    prime(sbufs, sload_sem, 2, experts - ahead, experts - late)
    send(2, experts - ahead, experts - late, low=half)

    for k in range(1, banks):
        r2(k).wait()
    out_router[...] = rt[...]
    for i in range(ahead - EARLY, ahead):
        early_free(i % EARLY)
    for t in range(late):
        for j in range(half):
            early_keep((ahead - late + t) % EARLY, t, j).wait()
    for i in range(ns):
        g = 3 * experts - late - ns + i
        free(g % ns, half if g >= turn else 1)
    for m in range(3):
        for k in range(1, n):
            count = experts if m < 2 else experts - ahead if k < half else experts - late
            whole = outs[m].at[pl.ds(0, count), :, pl.ds(0, rows)]
            pltpu.make_async_copy(whole, whole, recv_sem.at[m, k - 1]).wait()
    for k in range(1, half):
        whole = out_down.at[pl.ds(0, ahead), :, pl.ds(0, rows)]
        pltpu.make_async_copy(whole, whole, early_recv.at[k - 1]).wait()


def place_kernel(
    n, late, gate, up, down, router, out_gate, out_up, out_down, out_router, ring, in_sem, out_sem, router_sem
):
    experts, depth = gate.shape[0], ring.shape[0]
    half = gate.shape[2] // 2
    near = pl.ds(pl.multiple_of(lax.axis_index("zero") // (n // 2) * half, LANES), half)
    pairs = ((gate, out_gate), (up, out_up), (down, out_down))
    blocks = [(m, e) for m in range(3) for e in range(experts)]

    def views(i):
        m, e = blocks[i]
        if m == 2 and e >= experts - late:
            return pairs[m][0].at[e, :, near], ring.at[i % depth, :, pl.ds(0, half)], pairs[m][1].at[e, :, near]
        return pairs[m][0].at[e], ring.at[i % depth], pairs[m][1].at[e]

    def take(i):
        source, hold, _ = views(i)
        return pltpu.make_async_copy(source, hold, in_sem.at[i % depth])

    def put(i):
        _, hold, target = views(i)
        return pltpu.make_async_copy(hold, target, out_sem.at[i % depth])

    whole_router = pltpu.make_async_copy(router, out_router, router_sem)
    whole_router.start()
    lead = depth // 2
    for i in range(len(blocks) + lead):
        if i < len(blocks):
            if i >= depth:
                put(i - depth).wait()
            take(i).start()
        if i >= lead:
            take(i - lead).wait()
            put(i - lead).start()
    for i in range(max(0, len(blocks) - depth), len(blocks)):
        put(i).wait()
    whole_router.wait()


def late_kernel(*refs):
    *got, down, out, out_sem = refs
    half = len(got)
    late, _, rows = got[0].shape
    experts = down.shape[0]
    me = lax.axis_index("zero")

    def put(j):
        k = half + j
        bits = [i for i in range(k.bit_length()) if k & (1 << i)]
        p = me + sum((1 - 2 * lax.rem(me // (1 << i), 2)) * (1 << i) for i in bits)
        lanes = pl.ds(pl.multiple_of(p * rows, LANES), rows)
        return pltpu.make_async_copy(got[j], out.at[pl.ds(experts - late, late), :, lanes], out_sem.at[j])

    for j in range(half):
        put(j).start()
    for j in range(half):
        put(j).wait()


def fused_shards(n, banks, master_gate, master_up, master_down, router_weight, router_gain):
    experts, rows, width = master_gate.shape
    piece = width // n
    columns = router_weight.shape[1]
    units, first, late, ahead, half = 3 * experts, n // 2, LATE, AHEAD, n // 2
    levels = n.bit_length() - 1
    final = jax.ShapeDtypeStruct((experts, piece, n * rows), jnp.bfloat16)
    hbm, vmem = pl.BlockSpec(memory_space=pl.ANY), pl.BlockSpec(memory_space=pltpu.VMEM)
    dma = pltpu.SemaphoreType.DMA
    nx, ns = 4, SLOTS

    def halves(size):
        return tuple(
            pltpu.VMEM((size >> min(i + 1, levels - 1), 1, width), jnp.float32) for i in range(levels)
        )

    gate, up, down, *tails, scale, router = pl.pallas_call(
        functools.partial(exchange_kernel, n, banks, first, late, ahead),
        out_shape=[
            final,
            final,
            final,
            *[jax.ShapeDtypeStruct((late, piece, rows), jnp.bfloat16)] * half,
            jax.ShapeDtypeStruct((units, 1, width), jnp.float32),
            jax.ShapeDtypeStruct((banks * columns, n * rows), jnp.bfloat16),
        ],
        in_specs=[hbm] * 5,
        out_specs=[hbm] * (3 + half) + [vmem, vmem],
        scratch_shapes=[
            pltpu.VMEM((nx, rows, width), jnp.float32),
            pltpu.VMEM((nx, width, rows), jnp.float32),
            pltpu.VMEM((nx, rows, width), jnp.float32),
            pltpu.VMEM((nx, width, rows), jnp.float32),
            pltpu.VMEM((ns, width, rows), jnp.bfloat16),
            pltpu.VMEM((EARLY, width, rows), jnp.bfloat16),
            pltpu.VMEM((units, 1, width), jnp.float32),
            pltpu.VMEM((n - 1, 1, width), jnp.float32),
            pltpu.VMEM((first // 2, 1, width), jnp.float32),
            pltpu.VMEM((first // 2, 1, width), jnp.float32),
            pltpu.VMEM((half - 1, first // 2, 1, width), jnp.float32),
            pltpu.VMEM((first, 1, width), jnp.float32),
            pltpu.VMEM((units, 1, width), jnp.float32),
            pltpu.VMEM((columns, rows), jnp.float32),
            pltpu.VMEM((1, rows), jnp.float32),
            pltpu.VMEM((banks * columns, n * rows), jnp.bfloat16),
            halves(experts - first),
            halves(2 * experts),
            dma((2, nx)),
            dma((2, nx)),
            dma((ns, n - 1)),
            dma((ns,)),
            dma((EARLY, half + 1)),
            dma((EARLY, half - 1)),
            dma((half - 1,)),
            dma((3, n - 1)),
            dma((n - 1,)),
            dma((n - 1,)),
            dma((half + 1,)),
            dma((half + 1,)),
            dma((2, 2 * levels - 1)),
            dma((2, 2 * levels - 1)),
            dma((2,)),
            dma((half - 1,)),
            dma((half - 1,)),
            dma((half,)),
            dma((half,)),
            dma((banks - 1,)),
            dma((banks - 1,)),
        ],
        compiler_params=pltpu.CompilerParams(
            collective_id=0, has_side_effects=True, vmem_limit_bytes=56 * 1024 * 1024
        ),
    )(master_gate, master_up, master_down, router_weight.T, router_gain[None, :])
    got = [None] * half
    for j in reversed(range(half)):
        got[j] = lax.ppermute(tails[j], "zero", [(i, i ^ (half + j)) for i in range(n)])
    depth = 16
    moved = 2 * 2 * (3 * experts - late) * piece * n * rows
    final_gate, final_up, final_down, router = pl.pallas_call(
        functools.partial(place_kernel, n, late),
        out_shape=[final, final, final, jax.ShapeDtypeStruct(router.shape, router.dtype)],
        in_specs=[hbm] * 3 + [vmem],
        out_specs=[hbm] * 4,
        scratch_shapes=[
            pltpu.VMEM((depth, piece, n * rows), jnp.bfloat16),
            dma((depth,)),
            dma((depth,)),
            dma,
        ],
        compiler_params=pltpu.CompilerParams(vmem_limit_bytes=56 * 1024 * 1024),
        cost_estimate=pl.CostEstimate(flops=0, bytes_accessed=moved, transcendentals=0),
    )(gate, up, down, router)
    final_down = pl.pallas_call(
        late_kernel,
        out_shape=final,
        in_specs=[vmem] * half + [hbm],
        out_specs=hbm,
        input_output_aliases={half: 0},
        scratch_shapes=[dma((half,))],
        compiler_params=pltpu.CompilerParams(vmem_limit_bytes=8 * 1024 * 1024),
        cost_estimate=pl.CostEstimate(
            flops=0, bytes_accessed=4 * late * piece * n * rows, transcendentals=0
        ),
    )(*got, final_down)
    mine = lax.dynamic_slice_in_dim(
        scale.reshape(3, experts, width), lax.axis_index("zero") * piece, piece, axis=2
    )
    return (
        jnp.swapaxes(final_gate, 1, 2),
        jnp.swapaxes(final_up, 1, 2),
        final_down,
        mine[0],
        mine[1],
        mine[2],
        router.T,
    )


def shards(n, banks, *arrays):
    experts, rows, width = arrays[0].shape
    fits = (
        experts % n == 0
        and experts >= 2 * n
        and n == 1 << (n.bit_length() - 1)
        and rows % LANES == 0
        and width % LANES == 0
        and width // n % 16 == 0
        and arrays[3].shape[1] % 16 == 0
        and n == 8
        and banks > 1
    )
    return fused_shards(n, banks, *arrays) if fits else plain_shards(*arrays)


def solution(mesh):
    placed = (
        P("bank", "zero", None),
        P("bank", "zero", None),
        P("bank", None, "zero"),
        P("zero", "bank"),
        P("zero"),
    )
    return jax.shard_map(
        functools.partial(shards, mesh.shape["zero"], mesh.shape["bank"]),
        mesh=mesh,
        in_specs=placed,
        out_specs=(
            P("bank", None, "zero"),
            P("bank", None, "zero"),
            P("bank", "zero", None),
            P("bank", "zero"),
            P("bank", "zero"),
            P("bank", "zero"),
            P(),
        ),
        check_vma=False,
    )
```

```python
import functools

import jax
import jax.numpy as jnp
from jax import lax
from jax.experimental import pallas as pl
from jax.experimental.pallas import tpu as pltpu
from jax.sharding import PartitionSpec as P

MESH = pl.DeviceIdType.MESH
LANES = 128
LATE = 3
ROUTES = (3, 1, 0, 2)
AHEAD = 8
EARLY = 4
SLOTS = 3


def plain_shards(master_gate, master_up, master_down, router_weight, router_gain):
    scale_gate, scale_up, scale_down = lax.pmax(
        (
            jnp.max(jnp.abs(master_gate), axis=1),
            jnp.max(jnp.abs(master_up), axis=1),
            jnp.max(jnp.abs(master_down), axis=2),
        ),
        "zero",
    )
    narrow_gate, narrow_up, narrow_down = (
        (master_gate / jnp.expand_dims(scale_gate, 1)).astype(jnp.bfloat16),
        (master_up / jnp.expand_dims(scale_up, 1)).astype(jnp.bfloat16),
        (master_down / jnp.expand_dims(scale_down, 2)).astype(jnp.bfloat16),
    )
    final_gate, final_up = (
        lax.all_to_all(narrow_gate, "zero", split_axis=2, concat_axis=1, tiled=True),
        lax.all_to_all(narrow_up, "zero", split_axis=2, concat_axis=1, tiled=True),
    )
    final_down = lax.all_to_all(narrow_down, "zero", split_axis=1, concat_axis=2, tiled=True)
    scale_gate = lax.dynamic_slice_in_dim(
        scale_gate, lax.axis_index("zero") * final_gate.shape[2], final_gate.shape[2], axis=1
    )
    scale_up = lax.dynamic_slice_in_dim(
        scale_up, lax.axis_index("zero") * final_up.shape[2], final_up.shape[2], axis=1
    )
    scale_down = lax.dynamic_slice_in_dim(
        scale_down, lax.axis_index("zero") * final_down.shape[1], final_down.shape[1], axis=1
    )
    part_router = (router_weight * router_gain[:, None]).astype(jnp.bfloat16)
    row_router = lax.all_gather(part_router, "zero", axis=0, tiled=True)
    serve_router = lax.all_gather(row_router, "bank", axis=1, tiled=True)
    return (final_gate, final_up, final_down, scale_gate, scale_up, scale_down, serve_router)


def exchange_kernel(
    n, banks, first, late, ahead,
    gate, up, down, router, gain,
    out_gate, out_up, out_down, *rest,
):
    out_lates, rest = rest[: n // 2], rest[n // 2 :]
    exchange_body(n, banks, first, late, ahead, gate, up, down, router, gain, out_gate, out_up, out_down, out_lates, *rest)


def exchange_body(
    n, banks, first, late, ahead,
    gate, up, down, router, gain,
    out_gate, out_up, out_down, out_lates, out_scale, out_router,
    mrow, mcol, srow, scol, slots, early, partial, direct, pair_in, pair, pairs_in, quick, scale, rw, rg, rt, half_a, half_b,
    mload_sem, sload_sem, send_sem, local_sem, early_sem, early_send, early_recv, recv_sem,
    dx_send, dx_recv, q_send, q_recv, hx_send, hx_recv, r0_sem, r1_send, r1_recv, rx_send, rx_recv, r2_send, r2_recv,
):
    me = lax.axis_index("zero")
    bank = lax.axis_index("bank")
    experts, rows, width = gate.shape
    piece = width // n
    levels = len(half_a)
    nx, ns = mrow.shape[0], slots.shape[0]
    sources, outs = (gate, up, down), (out_gate, out_up, out_down)
    cols = router.shape[0]

    half = n // 2
    mine = pl.ds(pl.multiple_of(me * rows, LANES), rows)

    def flip(k):
        return me + sum((1 - 2 * lax.rem(me // (1 << i), 2)) * (k & (1 << i)) for i in range(levels))

    def bank_peer(k):
        return lax.rem(bank + k, banks)

    def load(bufs, sem, m, e):
        b = lax.rem(e, nx)
        return pltpu.make_async_copy(sources[m].at[e], bufs[m].at[b], sem.at[m // 2, b])

    def prime(bufs, sem, m, lo, hi):
        for i in range(min(nx - 1, hi - lo)):
            load(bufs, sem, m, lo + i).start()

    def stream(bufs, sem, m, lo, hi, end, body):
        def step(e, _):
            @pl.when(e + nx - 1 < end)
            def _():
                load(bufs, sem, m, e + nx - 1).start()

            body(e, bufs[m].at[lax.rem(e, nx)], load(bufs, sem, m, e))
            return 0

        lax.fori_loop(lo, hi, step, 0)

    mbufs, sbufs = (mrow, mrow, mcol), (srow, srow, scol)

    def maxima(m, lo, hi, end):
        def body(e, x, arrival):
            arrival.wait()
            u = m * experts + e
            if m < 2:
                partial[u] = jnp.max(jnp.abs(x[...]), axis=0, keepdims=True)
            else:
                top = jnp.abs(x[:, :LANES])
                for j in range(1, rows // LANES):
                    top = jnp.maximum(top, jnp.abs(x[:, j * LANES : (j + 1) * LANES]))
                partial[u] = jnp.max(top.T, axis=0, keepdims=True)

        stream(mbufs, mload_sem, m, lo, hi, end, body)

    def dx(k):
        return pltpu.make_async_remote_copy(
            src_ref=partial.at[0],
            dst_ref=direct.at[k - 1],
            send_sem=dx_send.at[k - 1],
            recv_sem=dx_recv.at[k - 1],
            device_id=(bank, flip(k)),
            device_id_type=MESH,
        )

    def dx_finish():
        top = partial[0]
        for k in range(1, n):
            dx(k).wait()
            top = jnp.maximum(top, direct[k - 1])
        scale[0] = top

    share = first // 2
    side = lax.rem(me, 2)
    ours = pl.ds(side * share, share)

    def qa():
        return pltpu.make_async_remote_copy(
            src_ref=partial.at[pl.ds((1 - side) * share, share)],
            dst_ref=pair_in,
            send_sem=q_send.at[0],
            recv_sem=q_recv.at[0],
            device_id=(bank, flip(1)),
            device_id_type=MESH,
        )

    def qb(i):
        return pltpu.make_async_remote_copy(
            src_ref=pair,
            dst_ref=pairs_in.at[i - 1],
            send_sem=q_send.at[i],
            recv_sem=q_recv.at[i],
            device_id=(bank, flip(2 * i)),
            device_id_type=MESH,
        )

    def qc():
        return pltpu.make_async_remote_copy(
            src_ref=quick.at[ours],
            dst_ref=quick.at[ours],
            send_sem=q_send.at[half],
            recv_sem=q_recv.at[half],
            device_id=(bank, flip(1)),
            device_id_type=MESH,
        )

    def quick_start():
        qa().wait()
        pair[...] = jnp.maximum(partial[ours], pair_in[...])
        for i in range(1, half):
            qb(i).start()

    def quick_finish():
        top = pair[...]
        for i in range(1, half):
            qb(i).wait()
            top = jnp.maximum(top, pairs_in[i - 1])
        quick[ours] = top
        qc().start()
        qc().wait()
        scale[pl.ds(1, first - 1)] = quick[pl.ds(1, first - 1)]

    def hx_ranges(lo, size):
        start, out = lo, []
        for i in range(levels - 1):
            part = size // 2
            bit = lax.rem(me // (1 << i), 2)
            out.append((start + bit * part, start + (1 - bit) * part, part))
            start, size = start + bit * part, part
        return out, start, size

    def hx(b, lo, size, stage):
        bufs = (half_a, half_b)[b]
        ranges, start, part = hx_ranges(lo, size)
        if stage < levels - 1:
            level = stage
            src, dst = partial.at[pl.ds(ranges[level][1], ranges[level][2])], bufs[level]
        elif stage == levels - 1:
            level = stage
            src, dst = partial.at[pl.ds(start, part)], bufs[level]
        else:
            level = 2 * (levels - 1) - stage
            src = scale.at[pl.ds(ranges[level][0], ranges[level][2])]
            dst = src
        bit = lax.rem(me // (1 << level), 2)
        return pltpu.make_async_remote_copy(
            src_ref=src,
            dst_ref=dst,
            send_sem=hx_send.at[b, stage],
            recv_sem=hx_recv.at[b, stage],
            device_id=(bank, me + (1 - 2 * bit) * (1 << level)),
            device_id_type=MESH,
        )

    def hx_start(b, lo, size, stage):
        hx(b, lo, size, stage).start()

    def hx_finish(b, lo, size, stage):
        bufs = (half_a, half_b)[b]
        hx(b, lo, size, stage).wait()
        ranges, start, part = hx_ranges(lo, size)
        if stage < levels - 1:
            keep = pl.ds(ranges[stage][0], ranges[stage][2])
            partial[keep] = jnp.maximum(partial[keep], bufs[stage][...])
        elif stage == levels - 1:
            scale[pl.ds(start, part)] = jnp.maximum(partial[pl.ds(start, part)], bufs[stage][...])

    def bulk(m, e, s, k):
        p = flip(k)
        return pltpu.make_async_remote_copy(
            src_ref=slots.at[s, pl.ds(pl.multiple_of(p * piece, 16), piece)],
            dst_ref=outs[m].at[e, :, pl.ds(pl.multiple_of(me * rows, LANES), rows)],
            send_sem=send_sem.at[s, k - 1],
            recv_sem=recv_sem.at[m, k - 1],
            device_id=(bank, p),
            device_id_type=MESH,
        )

    def own(m, e, s):
        return pltpu.make_async_copy(
            slots.at[s, pl.ds(pl.multiple_of(me * piece, 16), piece)],
            outs[m].at[e, :, pl.ds(pl.multiple_of(me * rows, LANES), rows)],
            local_sem.at[s],
        )

    def free(s, low=1):
        for k in range(low, n):
            bulk(0, 0, s, k).wait_send()
        if low == 1:
            own(0, 0, s).wait()

    def narrow(m, e, x, out):
        top = scale[m * experts + e]
        for j in range(width // LANES):
            cut = slice(j * LANES, (j + 1) * LANES)
            if m < 2:
                out[cut, :] = (x[:, cut] / top[:, cut]).T.astype(jnp.bfloat16)
            else:
                col = jnp.broadcast_to(top[:, cut], (LANES, LANES)).T
                for i in range(rows // LANES):
                    lane = slice(i * LANES, (i + 1) * LANES)
                    out[cut, lane] = (x[cut, lane] / col).astype(jnp.bfloat16)

    turn = 2 * experts + experts - ahead

    def send(m, lo, hi, before=None, after=None, low=1):
        def body(e, x, arrival):
            g = m * experts + e
            s = lax.rem(g, ns)

            @pl.when((g >= ns) & (g - ns < turn))
            def _():
                free(s)

            @pl.when(g - ns >= turn)
            def _():
                free(s, half)

            if before:
                before(e)
            arrival.wait()
            narrow(m, e, x, slots.at[s])
            for k in range(low, n):
                bulk(m, e, s, k).start()
            if low == 1:
                own(m, e, s).start()
            if after:
                after(e)

        stream(sbufs, sload_sem, m, lo, hi, hi, body)

    def route(q):
        return rt.at[pl.ds(pl.multiple_of(bank * cols, 16), cols), pl.ds(pl.multiple_of(q * rows, LANES), rows)]

    def r1(i):
        return pltpu.make_async_remote_copy(
            src_ref=route(me), dst_ref=route(me), send_sem=r1_send.at[i - 1], recv_sem=r1_recv.at[i - 1],
            device_id=(bank, flip(2 * i)), device_id_type=MESH,
        )

    def rx(i):
        q = flip(2 * i)
        return pltpu.make_async_remote_copy(
            src_ref=route(q), dst_ref=route(q), send_sem=rx_send.at[i], recv_sem=rx_recv.at[i],
            device_id=(bank, flip(1)), device_id_type=MESH,
        )

    def r2(k):
        mine = rt.at[pl.ds(pl.multiple_of(bank * cols, 16), cols)]
        return pltpu.make_async_remote_copy(
            src_ref=mine, dst_ref=mine, send_sem=r2_send.at[k - 1], recv_sem=r2_recv.at[k - 1],
            device_id=(bank_peer(k), me), device_id_type=MESH,
        )

    def r0():
        return pltpu.make_async_copy(router, rw, r0_sem.at[0]), pltpu.make_async_copy(gain, rg, r0_sem.at[1])

    prime(mbufs, mload_sem, 0, 0, experts)
    for copy in r0():
        copy.start()
    barrier = pltpu.get_barrier_semaphore()
    for k in range(1, n):
        pl.semaphore_signal(barrier, inc=1, device_id=(bank, flip(k)), device_id_type=MESH)
    for k in range(1, banks):
        pl.semaphore_signal(barrier, inc=1, device_id=(bank_peer(k), me), device_id_type=MESH)
    maxima(0, 0, 1, experts)
    for copy in r0():
        copy.wait()
    rt[pl.ds(pl.multiple_of(bank * cols, 16), cols), pl.ds(pl.multiple_of(me * rows, LANES), rows)] = (
        rw[...] * rg[...]
    ).astype(jnp.bfloat16)
    pl.semaphore_wait(barrier, n - 1 + banks - 1)
    for k in range(1, n):
        dx(k).start()
    for i in range(1, half):
        r1(i).start()
    prime(sbufs, sload_sem, 0, 0, experts)
    maxima(0, 1, first, experts)
    qa().start()
    quick_start()
    dx_finish()

    batches = ((0, first, experts - first), (1, experts, 2 * experts))
    last = 2 * (levels - 1)

    def before(e):
        @pl.when(e == 1)
        def _():
            maxima(0, first, experts, experts)
            quick_finish()
            hx_start(*batches[0], 0)
            hx_finish(*batches[0], 0)
            hx_start(*batches[0], 1)

        for stage in range(1, last):
            @pl.when(e == stage + 1)
            def _():
                hx_finish(*batches[0], stage)
                hx_start(*batches[0], stage + 1)
                if stage == last - 1:
                    hx_finish(*batches[0], last)

        @pl.when(e == first)
        def _():
            for i in range(1, half):
                r1(i).wait()
            for i in range(half):
                rx(i).start()

        @pl.when(e == first + 2)
        def _():
            for i in range(half):
                rx(i).wait()
            for k in range(1, banks):
                r2(k).start()

        for stage in range(last):
            @pl.when(e == 2 * (first + stage))
            def _():
                hx_finish(*batches[1], stage)
                hx_start(*batches[1], stage + 1)

        @pl.when(e == 2 * (first + last) - 1)
        def _():
            hx_finish(*batches[1], last)

    def after(e):
        for i in range(4):
            @pl.when(e == first + i)
            def _():
                m, lo = 1 + i // 2, (i % 2) * (experts // 2)
                hi = lo + experts // 2
                prime(mbufs, mload_sem, m, lo, hi)
                maxima(m, lo, hi, hi)

        @pl.when(e == first + 3)
        def _():
            hx_start(*batches[1], 0)

    send(0, 0, experts, before, after)
    prime(sbufs, sload_sem, 1, 0, experts)
    prime(sbufs, sload_sem, 2, experts - ahead, experts)

    def cut_of(b, p):
        return early.at[b, pl.ds(pl.multiple_of(p * piece, 16), piece)]

    def early_keep(b, t, j):
        return pltpu.make_async_copy(cut_of(b, flip(half + ROUTES[j])), out_lates[j].at[t], early_sem.at[b, j])

    def early_own(b, e):
        return pltpu.make_async_copy(cut_of(b, me), out_down.at[e, :, mine], early_sem.at[b, half])

    def early_near(b, e, k):
        return pltpu.make_async_remote_copy(
            src_ref=cut_of(b, flip(k)),
            dst_ref=out_down.at[e, :, mine],
            send_sem=early_send.at[b, k - 1],
            recv_sem=early_recv.at[k - 1],
            device_id=(bank, flip(k)),
            device_id_type=MESH,
        )

    def early_free(b):
        for k in range(1, half):
            early_near(b, 0, k).wait_send()
        early_own(b, 0).wait()

    def go_early(up_e):
        step = experts // ahead

        @pl.when(lax.rem(up_e, step) == step - 1)
        def _():
            i = up_e // step
            e = experts - ahead + i
            b = lax.rem(i, EARLY)

            @pl.when(i >= EARLY)
            def _():
                early_free(b)

            @pl.when(e + nx - 1 < experts)
            def _():
                load(sbufs, sload_sem, 2, e + nx - 1).start()

            load(sbufs, sload_sem, 2, e).wait()
            narrow(2, e, scol.at[lax.rem(e, nx)], early.at[b])
            for k in range(1, half):
                early_near(b, e, k).start()
            early_own(b, e).start()

            @pl.when(e >= experts - late)
            def _():
                for j in range(half):
                    early_keep(b, e - (experts - late), j).start()

    send(1, 0, experts, after=go_early)
    out_scale[...] = scale[...]
    prime(sbufs, sload_sem, 2, 0, experts - ahead)
    send(2, 0, experts - ahead)
    prime(sbufs, sload_sem, 2, experts - ahead, experts - late)
    send(2, experts - ahead, experts - late, low=half)

    for k in range(1, banks):
        r2(k).wait()
    out_router[...] = rt[...]
    for i in range(ahead - EARLY, ahead):
        early_free(i % EARLY)
    for t in range(late):
        for j in range(half):
            early_keep((ahead - late + t) % EARLY, t, j).wait()
    for i in range(ns):
        g = 3 * experts - late - ns + i
        free(g % ns, half if g >= turn else 1)
    for m in range(3):
        for k in range(1, n):
            count = experts if m < 2 else experts - ahead if k < half else experts - late
            whole = outs[m].at[pl.ds(0, count), :, pl.ds(0, rows)]
            pltpu.make_async_copy(whole, whole, recv_sem.at[m, k - 1]).wait()
    for k in range(1, half):
        whole = out_down.at[pl.ds(0, ahead), :, pl.ds(0, rows)]
        pltpu.make_async_copy(whole, whole, early_recv.at[k - 1]).wait()


def place_kernel(
    n, late, gate, up, down, router, out_gate, out_up, out_down, out_router, ring, in_sem, out_sem, router_sem
):
    experts, depth = gate.shape[0], ring.shape[0]
    half = gate.shape[2] // 2
    near = pl.ds(pl.multiple_of(lax.axis_index("zero") // (n // 2) * half, LANES), half)
    pairs = ((gate, out_gate), (up, out_up), (down, out_down))
    blocks = [(m, e) for m in range(3) for e in range(experts)]

    def views(i):
        m, e = blocks[i]
        if m == 2 and e >= experts - late:
            return pairs[m][0].at[e, :, near], ring.at[i % depth, :, pl.ds(0, half)], pairs[m][1].at[e, :, near]
        return pairs[m][0].at[e], ring.at[i % depth], pairs[m][1].at[e]

    def take(i):
        source, hold, _ = views(i)
        return pltpu.make_async_copy(source, hold, in_sem.at[i % depth])

    def put(i):
        _, hold, target = views(i)
        return pltpu.make_async_copy(hold, target, out_sem.at[i % depth])

    whole_router = pltpu.make_async_copy(router, out_router, router_sem)
    whole_router.start()
    lead = depth // 2
    for i in range(len(blocks) + lead):
        if i < len(blocks):
            if i >= depth:
                put(i - depth).wait()
            take(i).start()
        if i >= lead:
            take(i - lead).wait()
            put(i - lead).start()
    for i in range(max(0, len(blocks) - depth), len(blocks)):
        put(i).wait()
    whole_router.wait()


def late_kernel(*refs):
    *got, down, out, out_sem = refs
    half = len(got)
    late, _, rows = got[0].shape
    experts = down.shape[0]
    me = lax.axis_index("zero")

    def put(j):
        k = half + ROUTES[j]
        bits = [i for i in range(k.bit_length()) if k & (1 << i)]
        p = me + sum((1 - 2 * lax.rem(me // (1 << i), 2)) * (1 << i) for i in bits)
        lanes = pl.ds(pl.multiple_of(p * rows, LANES), rows)
        return pltpu.make_async_copy(got[j], out.at[pl.ds(experts - late, late), :, lanes], out_sem.at[j])

    for j in range(half):
        put(j).start()
    for j in range(half):
        put(j).wait()


def fused_shards(n, banks, master_gate, master_up, master_down, router_weight, router_gain):
    experts, rows, width = master_gate.shape
    piece = width // n
    columns = router_weight.shape[1]
    units, first, late, ahead, half = 3 * experts, n // 2, LATE, AHEAD, n // 2
    levels = n.bit_length() - 1
    final = jax.ShapeDtypeStruct((experts, piece, n * rows), jnp.bfloat16)
    hbm, vmem = pl.BlockSpec(memory_space=pl.ANY), pl.BlockSpec(memory_space=pltpu.VMEM)
    dma = pltpu.SemaphoreType.DMA
    nx, ns = 4, SLOTS

    def halves(size):
        return tuple(
            pltpu.VMEM((size >> min(i + 1, levels - 1), 1, width), jnp.float32) for i in range(levels)
        )

    gate, up, down, *tails, scale, router = pl.pallas_call(
        functools.partial(exchange_kernel, n, banks, first, late, ahead),
        out_shape=[
            final,
            final,
            final,
            *[jax.ShapeDtypeStruct((late, piece, rows), jnp.bfloat16)] * half,
            jax.ShapeDtypeStruct((units, 1, width), jnp.float32),
            jax.ShapeDtypeStruct((banks * columns, n * rows), jnp.bfloat16),
        ],
        in_specs=[hbm] * 5,
        out_specs=[hbm] * (3 + half) + [vmem, vmem],
        scratch_shapes=[
            pltpu.VMEM((nx, rows, width), jnp.float32),
            pltpu.VMEM((nx, width, rows), jnp.float32),
            pltpu.VMEM((nx, rows, width), jnp.float32),
            pltpu.VMEM((nx, width, rows), jnp.float32),
            pltpu.VMEM((ns, width, rows), jnp.bfloat16),
            pltpu.VMEM((EARLY, width, rows), jnp.bfloat16),
            pltpu.VMEM((units, 1, width), jnp.float32),
            pltpu.VMEM((n - 1, 1, width), jnp.float32),
            pltpu.VMEM((first // 2, 1, width), jnp.float32),
            pltpu.VMEM((first // 2, 1, width), jnp.float32),
            pltpu.VMEM((half - 1, first // 2, 1, width), jnp.float32),
            pltpu.VMEM((first, 1, width), jnp.float32),
            pltpu.VMEM((units, 1, width), jnp.float32),
            pltpu.VMEM((columns, rows), jnp.float32),
            pltpu.VMEM((1, rows), jnp.float32),
            pltpu.VMEM((banks * columns, n * rows), jnp.bfloat16),
            halves(experts - first),
            halves(2 * experts),
            dma((2, nx)),
            dma((2, nx)),
            dma((ns, n - 1)),
            dma((ns,)),
            dma((EARLY, half + 1)),
            dma((EARLY, half - 1)),
            dma((half - 1,)),
            dma((3, n - 1)),
            dma((n - 1,)),
            dma((n - 1,)),
            dma((half + 1,)),
            dma((half + 1,)),
            dma((2, 2 * levels - 1)),
            dma((2, 2 * levels - 1)),
            dma((2,)),
            dma((half - 1,)),
            dma((half - 1,)),
            dma((half,)),
            dma((half,)),
            dma((banks - 1,)),
            dma((banks - 1,)),
        ],
        compiler_params=pltpu.CompilerParams(
            collective_id=0, has_side_effects=True, vmem_limit_bytes=56 * 1024 * 1024
        ),
    )(master_gate, master_up, master_down, router_weight.T, router_gain[None, :])
    got = [
        lax.ppermute(tails[j], "zero", [(i, i ^ (half + ROUTES[j])) for i in range(n)]) for j in range(half)
    ]
    depth = 16
    moved = 2 * 2 * (3 * experts - late) * piece * n * rows
    final_gate, final_up, final_down, router = pl.pallas_call(
        functools.partial(place_kernel, n, late),
        out_shape=[final, final, final, jax.ShapeDtypeStruct(router.shape, router.dtype)],
        in_specs=[hbm] * 3 + [vmem],
        out_specs=[hbm] * 4,
        scratch_shapes=[
            pltpu.VMEM((depth, piece, n * rows), jnp.bfloat16),
            dma((depth,)),
            dma((depth,)),
            dma,
        ],
        compiler_params=pltpu.CompilerParams(vmem_limit_bytes=56 * 1024 * 1024),
        cost_estimate=pl.CostEstimate(flops=0, bytes_accessed=moved, transcendentals=0),
    )(gate, up, down, router)
    final_down = pl.pallas_call(
        late_kernel,
        out_shape=final,
        in_specs=[vmem] * half + [hbm],
        out_specs=hbm,
        input_output_aliases={half: 0},
        scratch_shapes=[dma((half,))],
        compiler_params=pltpu.CompilerParams(vmem_limit_bytes=8 * 1024 * 1024),
        cost_estimate=pl.CostEstimate(
            flops=0, bytes_accessed=4 * late * piece * n * rows, transcendentals=0
        ),
    )(*got, final_down)
    mine = lax.dynamic_slice_in_dim(
        scale.reshape(3, experts, width), lax.axis_index("zero") * piece, piece, axis=2
    )
    return (
        jnp.swapaxes(final_gate, 1, 2),
        jnp.swapaxes(final_up, 1, 2),
        final_down,
        mine[0],
        mine[1],
        mine[2],
        router.T,
    )


def shards(n, banks, *arrays):
    experts, rows, width = arrays[0].shape
    fits = (
        experts % n == 0
        and experts >= 2 * n
        and n == 1 << (n.bit_length() - 1)
        and rows % LANES == 0
        and width % LANES == 0
        and width // n % 16 == 0
        and arrays[3].shape[1] % 16 == 0
        and n == 8
        and banks > 1
    )
    return fused_shards(n, banks, *arrays) if fits else plain_shards(*arrays)


def solution(mesh):
    placed = (
        P("bank", "zero", None),
        P("bank", "zero", None),
        P("bank", None, "zero"),
        P("zero", "bank"),
        P("zero"),
    )
    return jax.shard_map(
        functools.partial(shards, mesh.shape["zero"], mesh.shape["bank"]),
        mesh=mesh,
        in_specs=placed,
        out_specs=(
            P("bank", None, "zero"),
            P("bank", None, "zero"),
            P("bank", "zero", None),
            P("bank", "zero"),
            P("bank", "zero"),
            P("bank", "zero"),
            P(),
        ),
        check_vma=False,
    )
```
